32 devices in a mesh: group: 8 (over z, core), member: 4 (over y, x).
Axes of the slice: x: 2, y: 2, z: 4, core: 2. Of those that a mesh axis runs over, the one named last changes fastest.
Arguments:
- source: float32 [256, 128, 128], P('group', 'member'), may hold values from -5 to 8
- potential: float32 [256, 128, 128], P('group', 'member'), may hold values from -3 to 3
- refined: int32 [8, 4, 4], P('group', 'member'), may hold values 0 or 1
Outputs:
- smoothed: float32 [256, 128, 128], P('group', 'member')
- residual: float32 [256, 128, 128], P('group', 'member')
The draws below stay inside these ranges and needn't reach their ends.
Inputs may be any that keep to these rules, and one draw needn't show every extreme that they name: 1 marks a refined box, 0 one that is not smoothed on the fine level.
All inputs are finite; a program needn't handle non-finite values. No bound on the sum of `refined` on one device may be relied on, other than what follows from the above.
Results may differ from the reference program's by a relative error of at most 0.000035.
Values sent between devices are 32-bit elements; how exact they have to be, the bound alone decides.
A program may use at most 128 MiB of HBM per device.

```python
import jax
import jax.numpy as jnp
from jax import lax

BOX = 32
NZB = 4
PRE = 2
POST = 2
COARSE = 2
NX = 256
NY = 128
NZ = 128
N_GROUP = 8
N_MEMBER = 4


def draw_source(key, part):
    key_noise = jax.random.fold_in(key, 11)
    shape = (NX, NY, NZ)
    along_x = lax.broadcasted_iota(jnp.float32, shape, 0) / (NX - 1.0)
    along_y = lax.broadcasted_iota(jnp.float32, shape, 1) / (NY - 1.0)
    noise = jnp.clip(jax.random.normal(key_noise, shape, jnp.float32), -4.0, 4.0)
    offset = 1.0 + along_x + along_y
    return (noise + offset).astype(jnp.float32)


def set_ends(entries, key, smallest, high):
    shape = entries.shape
    index_at = [jax.random.randint(jax.random.fold_in(key, axis), (), 0, shape[axis]) for axis in range(len(shape))]
    entries = entries.at[tuple(index_at)].set(smallest)
    longest = shape.index(max(shape))
    index_at[longest] = (index_at[longest] + 1) % shape[longest]
    return entries.at[tuple(index_at)].set(high)


def levels(key, dims, pieces, low, high):
    def one(axis_at, parts):
        draws = jax.random.uniform(jax.random.fold_in(jax.random.fold_in(key, 6), axis_at), (parts,), jnp.float32, low / len(pieces), high / len(pieces))
        return jnp.repeat(jnp.exp(draws), dims[axis_at] // parts).reshape((-1,) + (1,) * (len(dims) - axis_at - 1))

    gain = one(*pieces[0])
    for cut in pieces[1:]:
        gain = gain * one(*cut)
    return gain


def normal_values(stream_key, dims, deviation, most, shards=(), held_as=jnp.bfloat16):
    array = deviation * jax.random.normal(stream_key, dims, jnp.float32)
    if shards:
        array = array * levels(stream_key, dims, shards, -0.22, 0.18)
    return jnp.clip(array, -most, most).astype(held_as)


def setup_inputs(seed: int = 0) -> dict:
    keys = jax.random.split(jax.random.key(seed), 4)
    source = draw_source(jax.random.fold_in(keys[3], 71), 0)
    potential = normal_values(keys[1], (NX, NY, NZ), 0.5, 3.0, ((0, 8), (1, 4)), jnp.float32)
    refined = set_ends((jax.random.randint(keys[2], (N_GROUP, N_MEMBER, NZB), 0, 4) < 3).astype(jnp.int32), jax.random.fold_in(keys[2], 1), 0, 1)
    return {"source": source, "potential": potential, "refined": refined}


def neighbour_sum(grid_field):
    padded = jnp.pad(grid_field, 1)
    total = padded[2:, 1:-1, 1:-1] + padded[:-2, 1:-1, 1:-1]
    total = total + padded[1:-1, 2:, 1:-1] + padded[1:-1, :-2, 1:-1]
    return total + padded[1:-1, 1:-1, 2:] + padded[1:-1, 1:-1, :-2]


def expand(values_in, factor):
    size_a, size_b, size_c = values_in.shape
    wide = jnp.broadcast_to(values_in[:, None, :, None, :, None], (size_a, factor, size_b, factor, size_c, factor))
    return wide.reshape(size_a * factor, size_b * factor, size_c * factor)


def parity_of(shape):
    along_x = lax.broadcasted_iota(jnp.int32, shape, 0)
    along_y = lax.broadcasted_iota(jnp.int32, shape, 1)
    along_z = lax.broadcasted_iota(jnp.int32, shape, 2)
    return (along_x + along_y + along_z) % 2


def red_black(grid_field, right_side, active, parity):
    for colour in (0, 1):
        update = (right_side + neighbour_sum(grid_field)) / 6.0
        grid_field = jnp.where((parity == colour) & active, update, grid_field)
    return grid_field


def reference(source, potential, refined):
    density_mean = jnp.sum(source) / (NX * NY * NZ)
    contrast = source - density_mean
    active = expand(refined == 1, BOX)
    parity = parity_of(source.shape)
    phi = potential
    for _ in range(PRE):
        phi = red_black(phi, contrast, active, parity)
    fine_residual = contrast - (6.0 * phi - neighbour_sum(phi))
    size_a, size_b, size_c = fine_residual.shape
    coarse_source = fine_residual.reshape(size_a // 2, 2, size_b // 2, 2, size_c // 2, 2).sum(axis=(1, 3, 5)) * 0.5
    coarse_parity = parity_of(coarse_source.shape)
    correction = jnp.zeros(coarse_source.shape, jnp.float32)
    for _ in range(COARSE):
        correction = red_black(correction, coarse_source, True, coarse_parity)
    phi = phi + expand(correction, 2)
    for _ in range(POST):
        phi = red_black(phi, contrast, active, parity)
    residual = contrast - (6.0 * phi - neighbour_sum(phi))
    return phi, residual
```

```python
import functools

import jax
import jax.numpy as jnp
from jax import lax
from jax.experimental import pallas as pl
from jax.experimental.pallas import tpu as pltpu
from jax.sharding import PartitionSpec as P

PRE = 2
POST = 2
COARSE = 2
SWEEP_DEPTH = 2 * max(PRE, POST)
DEPTH = SWEEP_DEPTH + 1
COARSE_DEPTH = 2 * COARSE - 1 + (DEPTH + 1) // 2
ROW0 = 8 + SWEEP_DEPTH
COARSE_ROW0 = 16
SIDES = ((0, -1), (0, 1), (-1, -1), (-1, 1), (1, -1), (1, 1), (-1, 0), (1, 0))
MESH = pl.DeviceIdType.MESH


def slabs(side, count, offset, depth):
    if side == 0:
        return pl.ds(offset, count), pl.ds(offset, count)
    if side < 0:
        return pl.ds(offset, depth), pl.ds(offset + count, depth)
    return pl.ds(offset + count - depth, depth), pl.ds(offset - depth, depth)


def halo_slabs(side, count, offset, depth):
    return pl.ds(offset, count) if side == 0 else slabs(-side, count, offset, depth)[1]


def kernel(
    dims, sizes,
    refined_ref, source_ref, potential_ref,
    smoothed_ref, residual_ref,
    fine, rhs, post, coarse, corr, flags, weights, coarse_weights, pair_rows, wide_rows, res_rows,
    member_sums, group_sums,
    local_sem, send_sem, recv_sem, msum_send, msum_recv, gsum_send, gsum_recv,
):
    groups, members = dims
    cx, cy, cz = sizes
    hx, hy = cx // 2, cy // 2
    group_at = lax.axis_index("group")
    member_at = lax.axis_index("member")
    work = cy + 2 * SWEEP_DEPTH
    coarse_work = hy + 16
    own_rows = pl.ds(ROW0, cy)
    own_planes = pl.ds(DEPTH, cx)

    load_rhs = pltpu.make_async_copy(source_ref, rhs.at[own_planes, own_rows], local_sem.at[0])
    load_fine = pltpu.make_async_copy(potential_ref, fine.at[own_planes, own_rows], local_sem.at[1])
    load_rhs.start()
    load_fine.start()

    def there(dx, dy):
        ok = None
        for side, at, count in ((dx, group_at, groups), (dy, member_at, members)):
            if side == 0:
                continue
            here = at > 0 if side < 0 else at < count - 1
            ok = here if ok is None else ok & here
        return ok

    def device(dx, dy):
        return (group_at + dx, member_at + dy)

    barrier = pltpu.get_barrier_semaphore()
    for o in range(1, members):
        pl.semaphore_signal(barrier, inc=1, device_id=(group_at, lax.rem(member_at + o, members)), device_id_type=MESH)
    for o in range(1, groups):
        pl.semaphore_signal(barrier, inc=1, device_id=(lax.rem(group_at + o, groups), member_at), device_id_type=MESH)
    expected = jnp.int32(groups - 1 + members - 1)
    for dx, dy in SIDES:
        if dx and dy:
            @pl.when(there(dx, dy))
            def _():
                pl.semaphore_signal(barrier, inc=1, device_id=device(dx, dy), device_id_type=MESH)
            expected = expected + there(dx, dy).astype(jnp.int32)

    lane8 = lax.broadcasted_iota(jnp.int32, (8, cz), 1)
    boxes = refined_ref.shape[2]
    box = cz // boxes
    marks = jnp.zeros((8, cz), jnp.int32)
    for b in range(boxes):
        marks = jnp.where(lane8 // box == b, jnp.full((8, cz), refined_ref[0, 0, b], jnp.int32), marks)
    flags[1, 1] = (marks == 1).astype(jnp.float32)

    for dx, dy in SIDES:
        @pl.when(jnp.logical_not(there(dx, dy)))
        def _():
            flags[1 + dx, 1 + dy] = jnp.zeros((8, cz), jnp.float32)
            px = halo_slabs(dx, cx, DEPTH, DEPTH)
            py = halo_slabs(dy, cy, ROW0, DEPTH)
            blank = jnp.zeros((py.size, cz), jnp.float32)

            def clear(i, carry):
                fine[px.start + i, py, :] = blank
                post[px.start + i, py, :] = blank
                return carry

            lax.fori_loop(0, px.size, clear, 0)

    crow = lax.broadcasted_iota(jnp.int32, (coarse_work, cz), 0) - (COARSE_ROW0 - 8)
    clane = lax.broadcasted_iota(jnp.int32, (coarse_work, cz), 1)
    clow = jnp.where(member_at > 0, -COARSE_DEPTH, 0)
    chigh = jnp.where(member_at < members - 1, hy + COARSE_DEPTH, hy)
    cinside = (crow >= clow) & (crow < chigh)
    cbase = (crow + clane // 2) & 1
    for region in range(3):
        if region == 1:
            keep = cinside
        else:
            alive = there(region - 1, 0).astype(jnp.int32)
            keep = cinside & (jnp.full(crow.shape, alive, jnp.int32) == 1)
        for q in range(2):
            coarse_weights[region, q] = (keep & (cbase == q)).astype(jnp.float32)

    load_rhs.wait()

    def add_plane(i, acc):
        for t in range(cy // 8):
            acc = acc + rhs[DEPTH + i, pl.ds(ROW0 + 8 * t, 8), :]
        return acc

    member_sums[0] = lax.fori_loop(0, cx, add_plane, jnp.zeros((8, cz), jnp.float32))
    load_fine.wait()
    pl.semaphore_wait(barrier, expected)

    def sum_copies(slots, send, recv, count, target):
        return [
            pltpu.make_async_remote_copy(
                src_ref=slots.at[0], dst_ref=slots.at[o], send_sem=send.at[o], recv_sem=recv.at[o],
                device_id=target(o), device_id_type=MESH,
            )
            for o in range(1, count)
        ]

    msum = sum_copies(member_sums, msum_send, msum_recv, members, lambda o: (group_at, lax.rem(member_at + o, members)))
    gsum = sum_copies(group_sums, gsum_send, gsum_recv, groups, lambda o: (lax.rem(group_at + o, groups), member_at))
    for c in msum:
        c.start()

    def halo_copy(kind, n, src, dst, counts, offsets, depth):
        dx, dy = SIDES[n]
        sx, tx = slabs(dx, counts[0], offsets[0], depth)
        sy, ty = slabs(dy, counts[1], offsets[1], depth)
        return pltpu.make_async_remote_copy(
            src_ref=src.at[sx, sy], dst_ref=dst.at[tx, ty],
            send_sem=send_sem.at[kind, n], recv_sem=recv_sem.at[kind, n],
            device_id=device(dx, dy), device_id_type=MESH,
        )

    def first_round(n):
        dx, dy = SIDES[n]
        return [
            pltpu.make_async_remote_copy(
                src_ref=flags.at[1, 1], dst_ref=flags.at[1 - dx, 1 - dy],
                send_sem=send_sem.at[0, n], recv_sem=recv_sem.at[0, n],
                device_id=device(dx, dy), device_id_type=MESH,
            ),
            halo_copy(1, n, fine, fine, (cx, cy), (DEPTH, ROW0), DEPTH),
            halo_copy(2, n, rhs, rhs, (cx, cy), (DEPTH, ROW0), SWEEP_DEPTH),
        ]

    def second_coarse(n):
        return [halo_copy(3, n, coarse, coarse, (hx, hy), (COARSE_DEPTH, COARSE_ROW0), COARSE_DEPTH)]

    def second_fine(n):
        return [halo_copy(4, n, fine, post, (cx, cy), (DEPTH, ROW0), DEPTH)]

    def start(round_of):
        for n, (dx, dy) in enumerate(SIDES):
            @pl.when(there(dx, dy))
            def _():
                for c in round_of(n):
                    c.start()

    def arrive(round_of):
        for n, (dx, dy) in enumerate(SIDES):
            @pl.when(there(-dx, -dy))
            def _():
                for c in round_of(n):
                    c.wait_recv()

    def sent(round_of):
        for n, (dx, dy) in enumerate(SIDES):
            @pl.when(there(dx, dy))
            def _():
                for c in round_of(n):
                    c.wait_send()

    start(first_round)

    for c in msum:
        c.wait_recv()
    part = member_sums[0]
    for o in range(1, members):
        part = part + member_sums[o]
    group_sums[0] = part
    for c in gsum:
        c.start()
    for c in gsum:
        c.wait_recv()
    total = group_sums[0]
    for o in range(1, groups):
        total = total + group_sums[o]
    mean = jnp.sum(total) / (cx * cy * cz * groups * members)

    arrive(first_round)
    sent(first_round)

    frow = lax.broadcasted_iota(jnp.int32, (work, cz), 0) - SWEEP_DEPTH
    flane = lax.broadcasted_iota(jnp.int32, (work, cz), 1)
    fbase = (frow + flane) & 1
    for region in range(3):
        here = jnp.where(
            frow < 0, flags[region, 0, 0:1, :], jnp.where(frow < cy, flags[region, 1, 0:1, :], flags[region, 2, 0:1, :])
        )
        for q in range(2):
            weights[region, q] = jnp.where(fbase == q, here, 0.0)

    def lanes(value, step):
        lane = lax.broadcasted_iota(jnp.int32, value.shape, 1)
        low = jnp.where(lane < step, 0.0, pltpu.roll(value, step, 1))
        high = jnp.where(lane >= cz - step, 0.0, pltpu.roll(value, cz - step, 1))
        return low + high

    def around(field, i, row, rows, step):
        centre = field[i, pl.ds(row, rows), :]
        total = field[i - 1, pl.ds(row, rows), :] + field[i + 1, pl.ds(row, rows), :]
        total = total + (field[i, pl.ds(row - 1, rows), :] + field[i, pl.ds(row + 1, rows), :])
        return centre, total + lanes(centre, step)

    def smooth(field, count):
        for t in range(2 * count):
            reach = 2 * count - t

            def one(i, carry):
                region = (i >= DEPTH).astype(jnp.int32) + (i >= DEPTH + cx).astype(jnp.int32)
                parity = lax.rem(i + DEPTH + t, 2)
                centre, nbr = around(field, i, 8, work, 1)
                update = (rhs[i, pl.ds(8, work), :] - mean + nbr) * (1.0 / 6.0)
                field[i, pl.ds(8, work), :] = jnp.where(weights[region, parity] > 0.5, update, centre)
                return carry

            lax.fori_loop(DEPTH - reach, DEPTH + cx + reach, one, 0)

    smooth(fine, PRE)

    lane = lax.broadcasted_iota(jnp.int32, (cy, cz), 1)
    even = lane % 2 == 0

    def defect(field, i):
        centre, nbr = around(field, i, ROW0, cy, 1)
        return centre, rhs[i, own_rows, :] - mean - (6.0 * centre - nbr)

    def restrict(a, carry):
        i = DEPTH + 2 * a
        first, res_a = defect(fine, i)
        second, res_b = defect(fine, i + 1)
        post[i, own_rows, :] = first
        post[i + 1, own_rows, :] = second
        both = res_a + res_b
        both = both + jnp.where(even, pltpu.roll(both, cz - 1, 1), pltpu.roll(both, 1, 1))
        pair_rows[a] = both
        coarse[COARSE_DEPTH + a, pl.ds(COARSE_ROW0, hy), :] = 0.5 * (
            pair_rows[a, pl.ds(0, hy, stride=2), :] + pair_rows[a, pl.ds(1, hy, stride=2), :]
        )
        return carry

    lax.fori_loop(0, hx, restrict, 0)

    start(second_coarse)
    start(second_fine)
    arrive(second_coarse)
    sent(second_coarse)

    planes = hx + 2 * COARSE_DEPTH

    def coarse_region(i):
        return (i >= COARSE_DEPTH).astype(jnp.int32) + (i >= COARSE_DEPTH + hx).astype(jnp.int32)

    def coarse_first(i, carry):
        w = coarse_weights[coarse_region(i), lax.rem(i + COARSE_DEPTH, 2)]
        corr[i, pl.ds(8, coarse_work), :] = jnp.where(w > 0.5, coarse[i, pl.ds(8, coarse_work), :] * (1.0 / 6.0), 0.0)
        return carry

    lax.fori_loop(0, planes, coarse_first, 0)
    for t in range(1, 2 * COARSE):
        def coarse_one(i, carry):
            w = coarse_weights[coarse_region(i), lax.rem(i + COARSE_DEPTH + t, 2)]
            centre, nbr = around(corr, i, 8, coarse_work, 2)
            update = (coarse[i, pl.ds(8, coarse_work), :] + nbr) * (1.0 / 6.0)
            corr[i, pl.ds(8, coarse_work), :] = jnp.where(w > 0.5, update, centre)
            return carry

        lax.fori_loop(t, planes - t, coarse_one, 0)

    arrive(second_fine)
    sent(second_fine)

    half_rows = hy + 8
    first_plane = 2 * COARSE - 1

    def add_correction(c, carry):
        plane = corr[c, pl.ds(COARSE_ROW0 - 4, half_rows), :]
        wide_rows[c, pl.ds(0, half_rows, stride=2), :] = plane
        wide_rows[c, pl.ds(1, half_rows, stride=2), :] = plane
        wide = wide_rows[c]
        for b in range(2):
            i = 2 * (c - COARSE_DEPTH) + DEPTH + b
            post[i, pl.ds(ROW0 - 8, cy + 16), :] = post[i, pl.ds(ROW0 - 8, cy + 16), :] + wide
        return carry

    def add_end(c, b):
        plane = corr[c, pl.ds(COARSE_ROW0 - 4, half_rows), :]
        wide_rows[c, pl.ds(0, half_rows, stride=2), :] = plane
        wide_rows[c, pl.ds(1, half_rows, stride=2), :] = plane
        i = 2 * (c - COARSE_DEPTH) + DEPTH + b
        post[i, pl.ds(ROW0 - 8, cy + 16), :] = post[i, pl.ds(ROW0 - 8, cy + 16), :] + wide_rows[c]

    add_end(first_plane, 1)
    lax.fori_loop(first_plane + 1, planes - first_plane - 1, add_correction, 0)
    add_end(planes - first_plane - 1, 0)

    smooth(post, POST)
    store_smoothed = pltpu.make_async_copy(post.at[own_planes, own_rows], smoothed_ref, local_sem.at[0])
    store_smoothed.start()

    def last(i, carry):
        res_rows[i] = defect(post, DEPTH + i)[1]
        return carry

    lax.fori_loop(0, cx, last, 0)
    store_residual = pltpu.make_async_copy(res_rows, residual_ref, local_sem.at[1])
    store_residual.start()
    for c in msum + gsum:
        c.wait_send()
    store_smoothed.wait()
    store_residual.wait()


def per_device(dims, source, potential, refined):
    cx, cy, cz = source.shape
    groups, members = dims
    hx, hy = cx // 2, cy // 2
    wide = (cx + 2 * DEPTH, ROW0 + cy + ROW0, cz)
    narrow = (hx + 2 * COARSE_DEPTH, hy + 2 * COARSE_ROW0, cz)
    f32 = jnp.float32
    dma = pltpu.SemaphoreType.DMA
    any_spec = pl.BlockSpec(memory_space=pl.ANY)
    return tuple(pl.pallas_call(
        functools.partial(kernel, dims, (cx, cy, cz)),
        out_shape=[jax.ShapeDtypeStruct(source.shape, f32)] * 2,
        in_specs=[pl.BlockSpec(memory_space=pltpu.SMEM), any_spec, any_spec],
        out_specs=[any_spec, any_spec],
        scratch_shapes=[
            pltpu.VMEM(wide, f32),
            pltpu.VMEM(wide, f32),
            pltpu.VMEM(wide, f32),
            pltpu.VMEM(narrow, f32),
            pltpu.VMEM(narrow, f32),
            pltpu.VMEM((3, 3, 8, cz), f32),
            pltpu.VMEM((3, 2, cy + 2 * SWEEP_DEPTH, cz), f32),
            pltpu.VMEM((3, 2, hy + 16, cz), f32),
            pltpu.VMEM((hx, cy, cz), f32),
            pltpu.VMEM((narrow[0], cy + 16, cz), f32),
            pltpu.VMEM((cx, cy, cz), f32),
            pltpu.VMEM((members, 8, cz), f32),
            pltpu.VMEM((groups, 8, cz), f32),
            dma((2,)),
            dma((5, len(SIDES))),
            dma((5, len(SIDES))),
            dma((members,)),
            dma((members,)),
            dma((groups,)),
            dma((groups,)),
        ],
        compiler_params=pltpu.CompilerParams(collective_id=0, has_side_effects=True),
    )(refined, source, potential))


def solution(mesh):
    spec = P("group", "member", None)
    return jax.shard_map(
        functools.partial(per_device, (mesh.shape["group"], mesh.shape["member"])),
        mesh=mesh,
        in_specs=(spec, spec, spec),
        out_specs=(spec, spec),
        check_vma=False,
    )
```

```python
import functools

import jax
import jax.numpy as jnp
from jax import lax
from jax.experimental import pallas as pl
from jax.experimental.pallas import tpu as pltpu
from jax.sharding import PartitionSpec as P

PRE = 2
POST = 2
COARSE = 2
SWEEP_DEPTH = 2 * max(PRE, POST)
DEPTH = SWEEP_DEPTH + 1
COARSE_DEPTH = 2 * COARSE - 1 + (DEPTH + 1) // 2
ROW0 = 8 + SWEEP_DEPTH
COARSE_ROW0 = 16
GROUP = 8
STEPS = COARSE_DEPTH
SIDES = ((0, -1), (0, 1), (-1, -1), (-1, 1), (1, -1), (1, 1), (-1, 0), (1, 0))
MESH = pl.DeviceIdType.MESH


def slabs(side, count, offset, skip, depth):
    if side == 0:
        return pl.ds(offset, count), pl.ds(offset, count)
    if side < 0:
        return pl.ds(offset + skip, depth - skip), pl.ds(offset + count + skip, depth - skip)
    return pl.ds(offset + count - depth, depth - skip), pl.ds(offset - depth, depth - skip)


def corner_steps(depth):
    steps = []
    at = 0
    while at < depth - 1:
        width = 1 if (depth - 1 - at) % 2 else 2
        steps.append((at, at + width, depth - 1 - at))
        at += width
    return steps


def halo_slabs(side, count, offset, depth):
    return pl.ds(offset, count) if side == 0 else slabs(-side, count, offset, 0, depth)[1]


def region_of(at, offset, count):
    if isinstance(at, int):
        return int(at >= offset) + int(at >= offset + count)
    return (at >= offset).astype(jnp.int32) + (at >= offset + count).astype(jnp.int32)


def kernel(
    dims, sizes,
    refined_ref, source_ref, potential_ref,
    smoothed_ref, residual_ref,
    fine, rhs, post, coarse, corr, packed, flags, weights, coarse_weights, pair_rows, wide_rows, res_rows,
    member_sums, group_sums,
    local_sem, send_sem, recv_sem, msum_send, msum_recv, gsum_send, gsum_recv,
):
    groups, members = dims
    cx, cy, cz = sizes
    hx, hy = cx // 2, cy // 2
    group_at = lax.axis_index("group")
    member_at = lax.axis_index("member")
    work = cy + 2 * SWEEP_DEPTH
    coarse_work = hy + 16
    own_rows = pl.ds(ROW0, cy)
    own_planes = pl.ds(DEPTH, cx)

    load_rhs = pltpu.make_async_copy(source_ref, rhs.at[own_planes, own_rows], local_sem.at[0])
    load_fine = pltpu.make_async_copy(potential_ref, fine.at[own_planes, own_rows], local_sem.at[1])
    load_rhs.start()
    load_fine.start()

    def there(dx, dy):
        ok = None
        for side, at, count in ((dx, group_at, groups), (dy, member_at, members)):
            if side == 0:
                continue
            here = at > 0 if side < 0 else at < count - 1
            ok = here if ok is None else ok & here
        return ok

    def device(dx, dy):
        return (group_at + dx, member_at + dy)

    barrier = pltpu.get_barrier_semaphore()
    for o in range(1, members):
        pl.semaphore_signal(barrier, inc=1, device_id=(group_at, lax.rem(member_at + o, members)), device_id_type=MESH)
    for o in range(1, groups):
        pl.semaphore_signal(barrier, inc=1, device_id=(lax.rem(group_at + o, groups), member_at), device_id_type=MESH)
    expected = jnp.int32(groups - 1 + members - 1)
    for dx, dy in SIDES:
        if dx and dy:
            @pl.when(there(dx, dy))
            def _():
                pl.semaphore_signal(barrier, inc=1, device_id=device(dx, dy), device_id_type=MESH)
            expected = expected + there(dx, dy).astype(jnp.int32)

    lane8 = lax.broadcasted_iota(jnp.int32, (8, cz), 1)
    boxes = refined_ref.shape[2]
    box = cz // boxes
    marks = jnp.zeros((8, cz), jnp.int32)
    for b in range(boxes):
        marks = jnp.where(lane8 // box == b, jnp.full((8, cz), refined_ref[0, 0, b], jnp.int32), marks)
    flags[1, 1] = (marks == 1).astype(jnp.float32)

    for dx, dy in SIDES:
        @pl.when(jnp.logical_not(there(dx, dy)))
        def _():
            flags[1 + dx, 1 + dy] = jnp.zeros((8, cz), jnp.float32)
            px = halo_slabs(dx, cx, DEPTH, DEPTH)
            py = halo_slabs(dy, cy, ROW0, DEPTH)
            blank = jnp.zeros((py.size, cz), jnp.float32)

            def clear(i, carry):
                fine[px.start + i, py, :] = blank
                post[px.start + i, py, :] = blank
                return carry

            lax.fori_loop(0, px.size, clear, 0)

    crow = lax.broadcasted_iota(jnp.int32, (coarse_work, cz), 0) - (COARSE_ROW0 - 8)
    clane = lax.broadcasted_iota(jnp.int32, (coarse_work, cz), 1)
    clow = jnp.where(member_at > 0, -COARSE_DEPTH, 0)
    chigh = jnp.where(member_at < members - 1, hy + COARSE_DEPTH, hy)
    cinside = (crow >= clow) & (crow < chigh)
    cbase = (crow + clane // 2) & 1
    for region in range(3):
        if region == 1:
            keep = cinside
        else:
            alive = there(region - 1, 0).astype(jnp.int32)
            keep = cinside & (jnp.full(crow.shape, alive, jnp.int32) == 1)
        for q in range(2):
            coarse_weights[region, q] = (keep & (cbase == q)).astype(jnp.float32)

    load_rhs.wait()

    def add_plane(i, acc):
        for t in range(cy // 8):
            acc = acc + rhs[DEPTH + i, pl.ds(ROW0 + 8 * t, 8), :]
        return acc

    member_sums[0] = lax.fori_loop(0, cx, add_plane, jnp.zeros((8, cz), jnp.float32))
    load_fine.wait()
    pl.semaphore_wait(barrier, expected)

    def sum_copies(slots, send, recv, count, target):
        return [
            pltpu.make_async_remote_copy(
                src_ref=slots.at[0], dst_ref=slots.at[o], send_sem=send.at[o], recv_sem=recv.at[o],
                device_id=target(o), device_id_type=MESH,
            )
            for o in range(1, count)
        ]

    msum = sum_copies(member_sums, msum_send, msum_recv, members, lambda o: (group_at, lax.rem(member_at + o, members)))
    gsum = sum_copies(group_sums, gsum_send, gsum_recv, groups, lambda o: (lax.rem(group_at + o, groups), member_at))
    for c in msum:
        c.start()

    def halo_copies(kind, n, src, dst, counts, offsets, depth, skip=0):
        dx, dy = SIDES[n]
        steps = corner_steps(depth) if dx and dy else [(skip, depth, depth)]
        copies = []
        for m, (begin, end, reach) in enumerate(steps):
            sx, tx = slabs(dx, counts[0], offsets[0], begin, end)
            sy, ty = slabs(dy, counts[1], offsets[1], 0 if dx else skip, reach)
            copies.append(pltpu.make_async_remote_copy(
                src_ref=src.at[sx, sy], dst_ref=dst.at[tx, ty],
                send_sem=send_sem.at[kind + m, n], recv_sem=recv_sem.at[kind + m, n],
                device_id=device(dx, dy), device_id_type=MESH,
            ))
        return copies

    def first_round(n):
        dx, dy = SIDES[n]
        return [
            pltpu.make_async_remote_copy(
                src_ref=flags.at[1, 1], dst_ref=flags.at[1 - dx, 1 - dy],
                send_sem=send_sem.at[0, n], recv_sem=recv_sem.at[0, n],
                device_id=device(dx, dy), device_id_type=MESH,
            ),
        ] + (
            halo_copies(1, n, fine, fine, (cx, cy), (DEPTH, ROW0), DEPTH)
            + halo_copies(1 + STEPS, n, rhs, rhs, (cx, cy), (DEPTH, ROW0), SWEEP_DEPTH)
        )

    half_planes = hx // 2

    def second_coarse(n):
        dx, dy = SIDES[n]
        if dx:
            return halo_copies(1 + 2 * STEPS, n, coarse, coarse, (hx, hy), (COARSE_DEPTH, COARSE_ROW0), COARSE_DEPTH)
        return [pltpu.make_async_remote_copy(
            src_ref=packed.at[1 + dy, pl.ds(0, half_planes)], dst_ref=packed.at[1 + dy, pl.ds(half_planes, half_planes)],
            send_sem=send_sem.at[1 + 2 * STEPS, n], recv_sem=recv_sem.at[1 + 2 * STEPS, n],
            device_id=device(dx, dy), device_id_type=MESH,
        )]

    def second_fine(n):
        return halo_copies(1 + 3 * STEPS, n, fine, post, (cx, cy), (DEPTH, ROW0), DEPTH, 1)

    def start(round_of):
        for n, (dx, dy) in enumerate(SIDES):
            @pl.when(there(dx, dy))
            def _():
                for c in round_of(n):
                    c.start()

    def arrive(round_of):
        for n, (dx, dy) in enumerate(SIDES):
            @pl.when(there(-dx, -dy))
            def _():
                for c in round_of(n):
                    c.wait_recv()

    def sent(round_of):
        for n, (dx, dy) in enumerate(SIDES):
            @pl.when(there(dx, dy))
            def _():
                for c in round_of(n):
                    c.wait_send()

    start(first_round)

    for c in msum:
        c.wait_recv()
    part = member_sums[0]
    for o in range(1, members):
        part = part + member_sums[o]
    group_sums[0] = part
    for c in gsum:
        c.start()
    for c in gsum:
        c.wait_recv()
    total = group_sums[0]
    for o in range(1, groups):
        total = total + group_sums[o]
    mean = jnp.sum(total) / (cx * cy * cz * groups * members)

    arrive(first_round)
    sent(first_round)

    frow = lax.broadcasted_iota(jnp.int32, (work, cz), 0) - SWEEP_DEPTH
    flane = lax.broadcasted_iota(jnp.int32, (work, cz), 1)
    fbase = (frow + flane) & 1
    for region in range(3):
        here = jnp.where(
            frow < 0, flags[region, 0, 0:1, :], jnp.where(frow < cy, flags[region, 1, 0:1, :], flags[region, 2, 0:1, :])
        )
        for q in range(2):
            weights[region, q] = jnp.where(fbase == q, here, 0.0)

    def lanes(value, step):
        lane = lax.broadcasted_iota(jnp.int32, value.shape, 1)
        low = jnp.where(lane < step, 0.0, pltpu.roll(value, step, 1))
        high = jnp.where(lane >= cz - step, 0.0, pltpu.roll(value, cz - step, 1))
        return low + high

    def stencil(field, i, count, row, rows, step):
        planes = [field[i + k, pl.ds(row, rows), :] for k in range(-1, count + 1)]
        sums = []
        for k in range(count):
            total = planes[k] + planes[k + 2] + lanes(planes[k + 1], step)
            total = total + (field[i + k, pl.ds(row - 1, rows), :] + field[i + k, pl.ds(row + 1, rows), :])
            sums.append(total)
        return planes[1:-1], sums

    def in_groups(low, high, size, one):
        whole = (high - low) // size

        def body(g, carry):
            one(low + g * size, size, low)
            return carry

        lax.fori_loop(0, whole, body, 0)
        if (high - low) % size:
            one(low + whole * size, (high - low) % size, low)

    def smooth(field, count):
        for t in range(2 * count):
            reach = 2 * count - t

            def one(i, size, low):
                centres, sums = stencil(field, i, size, 8, work, 1)
                fresh = []
                for k in range(size):
                    at = i + k
                    mask = weights[region_of(at, DEPTH, cx), (low + k + DEPTH + t) % 2] > 0.5
                    update = (rhs[at, pl.ds(8, work), :] - mean + sums[k]) * (1.0 / 6.0)
                    fresh.append(jnp.where(mask, update, centres[k]))
                for k in range(size):
                    field[i + k, pl.ds(8, work), :] = fresh[k]

            in_groups(DEPTH - reach, DEPTH + cx + reach, GROUP, one)

    smooth(fine, PRE)

    lane = lax.broadcasted_iota(jnp.int32, (cy, cz), 1)
    even = lane % 2 == 0

    def defects(field, i, count):
        centres, sums = stencil(field, i, count, ROW0, cy, 1)
        return centres, [rhs[i + k, own_rows, :] - mean - (6.0 * centres[k] - sums[k]) for k in range(count)]

    def restrict(a, size, low):
        i = DEPTH + 2 * a
        centres, res = defects(fine, i, 2 * size)
        for k in range(size):
            both = res[2 * k] + res[2 * k + 1]
            both = both + jnp.where(even, pltpu.roll(both, cz - 1, 1), pltpu.roll(both, 1, 1))
            pair_rows[a + k] = both
        for k in range(2 * size):
            post[i + k, own_rows, :] = centres[k]
            post[i + k, pl.ds(ROW0 - 1, 1), :] = fine[i + k, pl.ds(ROW0 - 1, 1), :]
            post[i + k, pl.ds(ROW0 + cy, 1), :] = fine[i + k, pl.ds(ROW0 + cy, 1), :]
        for k in range(size):
            coarse[COARSE_DEPTH + a + k, pl.ds(COARSE_ROW0, hy), :] = 0.5 * (
                pair_rows[a + k, pl.ds(0, hy, stride=2), :] + pair_rows[a + k, pl.ds(1, hy, stride=2), :]
            )

    in_groups(0, hx, 2, restrict)

    leven = lax.broadcasted_iota(jnp.int32, (COARSE_DEPTH, cz), 1) % 2 == 0
    for dy in (-1, 1):
        sy = slabs(dy, hy, COARSE_ROW0, 0, COARSE_DEPTH)[0]
        for k in range(half_planes):
            packed[1 + dy, k] = jnp.where(
                leven, coarse[COARSE_DEPTH + k, sy, :], coarse[COARSE_DEPTH + half_planes + k, sy, :]
            )

    start(second_coarse)
    for i in (DEPTH - 1, DEPTH + cx):
        post[i, own_rows, :] = fine[i, own_rows, :]
    start(second_fine)
    arrive(second_coarse)
    sent(second_coarse)
    for dy in (-1, 1):
        ty = slabs(dy, hy, COARSE_ROW0, 0, COARSE_DEPTH)[1]

        @pl.when(there(0, -dy))
        def _():
            for k in range(half_planes):
                both = packed[1 + dy, half_planes + k]
                coarse[COARSE_DEPTH + k, ty, :] = jnp.where(leven, both, pltpu.roll(both, 1, 1))
                coarse[COARSE_DEPTH + half_planes + k, ty, :] = jnp.where(leven, pltpu.roll(both, cz - 1, 1), both)

    planes = hx + 2 * COARSE_DEPTH

    def coarse_mask(at, parity):
        return coarse_weights[region_of(at, COARSE_DEPTH, hx), parity % 2] > 0.5

    def coarse_first(i, size, low):
        for k in range(size):
            start_value = coarse[i + k, pl.ds(8, coarse_work), :] * (1.0 / 6.0)
            mask = coarse_mask(i + k, low + k + COARSE_DEPTH)
            corr[i + k, pl.ds(8, coarse_work), :] = jnp.where(mask, start_value, 0.0)

    in_groups(0, planes, GROUP, coarse_first)
    for t in range(1, 2 * COARSE):
        def coarse_one(i, size, low):
            centres, sums = stencil(corr, i, size, 8, coarse_work, 2)
            fresh = []
            for k in range(size):
                update = (coarse[i + k, pl.ds(8, coarse_work), :] + sums[k]) * (1.0 / 6.0)
                fresh.append(jnp.where(coarse_mask(i + k, low + k + COARSE_DEPTH + t), update, centres[k]))
            for k in range(size):
                corr[i + k, pl.ds(8, coarse_work), :] = fresh[k]

        in_groups(t, planes - t, GROUP, coarse_one)

    arrive(second_fine)
    sent(second_fine)

    half_rows = hy + 8
    first_plane = 2 * COARSE - 1

    def add_correction(c, size, low, sides=(0, 1)):
        for k in range(size):
            plane = corr[c + k, pl.ds(COARSE_ROW0 - 4, half_rows), :]
            wide_rows[c + k, pl.ds(0, half_rows, stride=2), :] = plane
            wide_rows[c + k, pl.ds(1, half_rows, stride=2), :] = plane
        rows = pl.ds(ROW0 - 8, cy + 16)
        fresh = []
        for k in range(size):
            wide = wide_rows[c + k]
            for b in sides:
                i = 2 * (c + k - COARSE_DEPTH) + DEPTH + b
                fresh.append((i, post[i, rows, :] + wide))
        for i, value in fresh:
            post[i, rows, :] = value

    add_correction(first_plane, 1, 0, (1,))
    in_groups(first_plane + 1, planes - first_plane - 1, 2, add_correction)
    add_correction(planes - first_plane - 1, 1, 0, (0,))

    smooth(post, POST)
    store_smoothed = pltpu.make_async_copy(post.at[own_planes, own_rows], smoothed_ref, local_sem.at[0])
    store_smoothed.start()

    def last(i, size, low):
        for k, value in enumerate(defects(post, DEPTH + i, size)[1]):
            res_rows[i + k] = value

    in_groups(0, cx, GROUP, last)
    store_residual = pltpu.make_async_copy(res_rows, residual_ref, local_sem.at[1])
    store_residual.start()
    for c in msum + gsum:
        c.wait_send()
    store_smoothed.wait()
    store_residual.wait()


def per_device(dims, source, potential, refined):
    cx, cy, cz = source.shape
    groups, members = dims
    hx, hy = cx // 2, cy // 2
    wide = (cx + 2 * DEPTH, ROW0 + cy + ROW0, cz)
    narrow = (hx + 2 * COARSE_DEPTH, hy + 2 * COARSE_ROW0, cz)
    f32 = jnp.float32
    dma = pltpu.SemaphoreType.DMA
    any_spec = pl.BlockSpec(memory_space=pl.ANY)
    return tuple(pl.pallas_call(
        functools.partial(kernel, dims, (cx, cy, cz)),
        out_shape=[jax.ShapeDtypeStruct(source.shape, f32)] * 2,
        in_specs=[pl.BlockSpec(memory_space=pltpu.SMEM), any_spec, any_spec],
        out_specs=[any_spec, any_spec],
        scratch_shapes=[
            pltpu.VMEM(wide, f32),
            pltpu.VMEM(wide, f32),
            pltpu.VMEM(wide, f32),
            pltpu.VMEM(narrow, f32),
            pltpu.VMEM(narrow, f32),
            pltpu.VMEM((3, 2 * (hx // 2), COARSE_DEPTH, cz), f32),
            pltpu.VMEM((3, 3, 8, cz), f32),
            pltpu.VMEM((3, 2, cy + 2 * SWEEP_DEPTH, cz), f32),
            pltpu.VMEM((3, 2, hy + 16, cz), f32),
            pltpu.VMEM((hx, cy, cz), f32),
            pltpu.VMEM((narrow[0], cy + 16, cz), f32),
            pltpu.VMEM((cx, cy, cz), f32),
            pltpu.VMEM((members, 8, cz), f32),
            pltpu.VMEM((groups, 8, cz), f32),
            dma((2,)),
            dma((1 + 4 * STEPS, len(SIDES))),
            dma((1 + 4 * STEPS, len(SIDES))),
            dma((members,)),
            dma((members,)),
            dma((groups,)),
            dma((groups,)),
        ],
        compiler_params=pltpu.CompilerParams(collective_id=0, has_side_effects=True),
    )(refined, source, potential))


def solution(mesh):
    spec = P("group", "member", None)
    return jax.shard_map(
        functools.partial(per_device, (mesh.shape["group"], mesh.shape["member"])),
        mesh=mesh,
        in_specs=(spec, spec, spec),
        out_specs=(spec, spec),
        check_vma=False,
    )
```

```python
import functools

import jax
import jax.numpy as jnp
from jax import lax
from jax.experimental import pallas as pl
from jax.experimental.pallas import tpu as pltpu
from jax.sharding import PartitionSpec as P

PRE = 2
POST = 2
COARSE = 2
SWEEP_DEPTH = 2 * max(PRE, POST)
DEPTH = SWEEP_DEPTH + 1
COARSE_DEPTH = 2 * COARSE - 1 + (DEPTH + 1) // 2
ROW0 = 8 + SWEEP_DEPTH
COARSE_ROW0 = 16
GROUP = 8
STEPS = COARSE_DEPTH
SIDES = ((0, -1), (0, 1), (-1, -1), (-1, 1), (1, -1), (1, 1), (-1, 0), (1, 0))
MESH = pl.DeviceIdType.MESH


def slabs(side, count, offset, skip, depth):
    if side == 0:
        return pl.ds(offset, count), pl.ds(offset, count)
    if side < 0:
        return pl.ds(offset + skip, depth - skip), pl.ds(offset + count + skip, depth - skip)
    return pl.ds(offset + count - depth, depth - skip), pl.ds(offset - depth, depth - skip)


def corner_steps(depth):
    steps = []
    at = 0
    while at < depth - 1:
        width = 1 if (depth - 1 - at) % 2 else 2
        steps.append((at, at + width, depth - 1 - at))
        at += width
    return steps


def halo_slabs(side, count, offset, depth):
    return pl.ds(offset, count) if side == 0 else slabs(-side, count, offset, 0, depth)[1]


def region_of(at, offset, count):
    if isinstance(at, int):
        return int(at >= offset) + int(at >= offset + count)
    return (at >= offset).astype(jnp.int32) + (at >= offset + count).astype(jnp.int32)


def kernel(
    dims, sizes,
    refined_ref, source_ref, potential_ref,
    smoothed_ref, residual_ref,
    fine, rhs, post, coarse, corr, packed, flags, weights, coarse_weights, pair_rows, wide_rows, res_rows,
    member_sums, group_sums,
    local_sem, send_sem, recv_sem, msum_send, msum_recv, gsum_send, gsum_recv,
):
    groups, members = dims
    cx, cy, cz = sizes
    hx, hy = cx // 2, cy // 2
    group_at = lax.axis_index("group")
    member_at = lax.axis_index("member")
    work = cy + 2 * SWEEP_DEPTH
    coarse_work = hy + 16
    own_rows = pl.ds(ROW0, cy)
    own_planes = pl.ds(DEPTH, cx)

    load_rhs = pltpu.make_async_copy(source_ref, rhs.at[own_planes, own_rows], local_sem.at[0])
    load_fine = pltpu.make_async_copy(potential_ref, fine.at[own_planes, own_rows], local_sem.at[1])
    load_sent = pltpu.make_async_copy(potential_ref, res_rows, local_sem.at[2])
    load_rhs.start()
    load_sent.start()
    load_fine.start()

    def there(dx, dy):
        ok = None
        for side, at, count in ((dx, group_at, groups), (dy, member_at, members)):
            if side == 0:
                continue
            here = at > 0 if side < 0 else at < count - 1
            ok = here if ok is None else ok & here
        return ok

    def device(dx, dy):
        return (group_at + dx, member_at + dy)

    barrier = pltpu.get_barrier_semaphore()
    for o in range(1, members):
        pl.semaphore_signal(barrier, inc=1, device_id=(group_at, lax.rem(member_at + o, members)), device_id_type=MESH)
    for o in range(1, groups):
        pl.semaphore_signal(barrier, inc=1, device_id=(lax.rem(group_at + o, groups), member_at), device_id_type=MESH)
    expected = jnp.int32(groups - 1 + members - 1)
    for dx, dy in SIDES:
        if dx and dy:
            @pl.when(there(dx, dy))
            def _():
                pl.semaphore_signal(barrier, inc=1, device_id=device(dx, dy), device_id_type=MESH)
            expected = expected + there(dx, dy).astype(jnp.int32)

    lane8 = lax.broadcasted_iota(jnp.int32, (8, cz), 1)
    boxes = refined_ref.shape[2]
    box = cz // boxes
    marks = jnp.zeros((8, cz), jnp.int32)
    for b in range(boxes):
        marks = jnp.where(lane8 // box == b, jnp.full((8, cz), refined_ref[0, 0, b], jnp.int32), marks)
    flags[1, 1] = (marks == 1).astype(jnp.float32)

    for dx, dy in SIDES:
        @pl.when(jnp.logical_not(there(dx, dy)))
        def _():
            flags[1 + dx, 1 + dy] = jnp.zeros((8, cz), jnp.float32)
            px = halo_slabs(dx, cx, DEPTH, DEPTH)
            py = halo_slabs(dy, cy, ROW0, DEPTH)
            blank = jnp.zeros((py.size, cz), jnp.float32)

            def clear(i, carry):
                fine[px.start + i, py, :] = blank
                post[px.start + i, py, :] = blank
                return carry

            lax.fori_loop(0, px.size, clear, 0)

    crow = lax.broadcasted_iota(jnp.int32, (coarse_work, cz), 0) - (COARSE_ROW0 - 8)
    clane = lax.broadcasted_iota(jnp.int32, (coarse_work, cz), 1)
    clow = jnp.where(member_at > 0, -COARSE_DEPTH, 0)
    chigh = jnp.where(member_at < members - 1, hy + COARSE_DEPTH, hy)
    cinside = (crow >= clow) & (crow < chigh)
    cbase = (crow + clane // 2) & 1
    for region in range(3):
        if region == 1:
            keep = cinside
        else:
            alive = there(region - 1, 0).astype(jnp.int32)
            keep = cinside & (jnp.full(crow.shape, alive, jnp.int32) == 1)
        for q in range(2):
            coarse_weights[region, q] = (keep & (cbase == q)).astype(jnp.float32)

    load_rhs.wait()

    def add_plane(i, acc):
        for t in range(cy // 8):
            acc = acc + rhs[DEPTH + i, pl.ds(ROW0 + 8 * t, 8), :]
        return acc

    member_sums[0] = lax.fori_loop(0, cx, add_plane, jnp.zeros((8, cz), jnp.float32))
    load_sent.wait()
    load_fine.wait()
    pl.semaphore_wait(barrier, expected)

    def sum_copies(slots, send, recv, count, target):
        return [
            pltpu.make_async_remote_copy(
                src_ref=slots.at[0], dst_ref=slots.at[o], send_sem=send.at[o], recv_sem=recv.at[o],
                device_id=target(o), device_id_type=MESH,
            )
            for o in range(1, count)
        ]

    msum = sum_copies(member_sums, msum_send, msum_recv, members, lambda o: (group_at, lax.rem(member_at + o, members)))
    gsum = sum_copies(group_sums, gsum_send, gsum_recv, groups, lambda o: (lax.rem(group_at + o, groups), member_at))
    for c in msum:
        c.start()

    def halo_copies(kind, n, src, dst, counts, offsets, depth, skip=0, base=None):
        dx, dy = SIDES[n]
        steps = corner_steps(depth) if dx and dy else [(skip, depth, depth)]
        copies = []
        for m, (begin, end, reach) in enumerate(steps):
            sx, tx = slabs(dx, counts[0], offsets[0], begin, end)
            sy, ty = slabs(dy, counts[1], offsets[1], 0 if dx else skip, reach)
            if base is not None:
                sx = pl.ds(sx.start - offsets[0] + base, sx.size)
                sy = pl.ds(sy.start - offsets[1] + base, sy.size)
            copies.append(pltpu.make_async_remote_copy(
                src_ref=src.at[sx, sy], dst_ref=dst.at[tx, ty],
                send_sem=send_sem.at[kind + m, n], recv_sem=recv_sem.at[kind + m, n],
                device_id=device(dx, dy), device_id_type=MESH,
            ))
        return copies

    def first_round(n):
        dx, dy = SIDES[n]
        return [
            pltpu.make_async_remote_copy(
                src_ref=flags.at[1, 1], dst_ref=flags.at[1 - dx, 1 - dy],
                send_sem=send_sem.at[0, n], recv_sem=recv_sem.at[0, n],
                device_id=device(dx, dy), device_id_type=MESH,
            ),
        ] + (
            halo_copies(1, n, res_rows, fine, (cx, cy), (DEPTH, ROW0), DEPTH, 0, 0)
            + halo_copies(1 + STEPS, n, rhs, rhs, (cx, cy), (DEPTH, ROW0), SWEEP_DEPTH)
        )

    half_planes = hx // 2

    def second_coarse(n):
        dx, dy = SIDES[n]
        if dx:
            return halo_copies(1 + 2 * STEPS, n, coarse, coarse, (hx, hy), (COARSE_DEPTH, COARSE_ROW0), COARSE_DEPTH)
        return [pltpu.make_async_remote_copy(
            src_ref=packed.at[1 + dy, pl.ds(0, half_planes)], dst_ref=packed.at[1 + dy, pl.ds(half_planes, half_planes)],
            send_sem=send_sem.at[1 + 2 * STEPS, n], recv_sem=recv_sem.at[1 + 2 * STEPS, n],
            device_id=device(dx, dy), device_id_type=MESH,
        )]

    def second_fine(n):
        return halo_copies(1 + 3 * STEPS, n, fine, post, (cx, cy), (DEPTH, ROW0), DEPTH, 1)

    def start(round_of):
        for n, (dx, dy) in enumerate(SIDES):
            @pl.when(there(dx, dy))
            def _():
                for c in round_of(n):
                    c.start()

    def arrive(round_of, sides=SIDES):
        for n, (dx, dy) in enumerate(SIDES):
            if (dx, dy) not in sides:
                continue

            @pl.when(there(-dx, -dy))
            def _():
                for c in round_of(n):
                    c.wait_recv()

    def sent(round_of):
        for n, (dx, dy) in enumerate(SIDES):
            @pl.when(there(dx, dy))
            def _():
                for c in round_of(n):
                    c.wait_send()

    start(first_round)

    for c in msum:
        c.wait_recv()
    part = member_sums[0]
    for o in range(1, members):
        part = part + member_sums[o]
    group_sums[0] = part
    for c in gsum:
        c.start()
    for c in gsum:
        c.wait_recv()
    total = group_sums[0]
    for o in range(1, groups):
        total = total + group_sums[o]
    mean = jnp.sum(total) / (cx * cy * cz * groups * members)

    along = ((-1, 0), (1, 0))
    arrive(first_round, along)

    def fine_masks(row, rows, member):
        frow = lax.broadcasted_iota(jnp.int32, (rows, cz), 0) + row
        flane = lax.broadcasted_iota(jnp.int32, (rows, cz), 1)
        fbase = (frow + flane) & 1
        for region in range(3):
            here = flags[region, member, 0:1, :]
            for q in range(2):
                weights[region, q, pl.ds(SWEEP_DEPTH + row, rows), :] = jnp.where(fbase == q, here, 0.0)

    fine_masks(0, cy, 1)

    def lanes(value, step):
        lane = lax.broadcasted_iota(jnp.int32, value.shape, 1)
        low = jnp.where(lane < step, 0.0, pltpu.roll(value, step, 1))
        high = jnp.where(lane >= cz - step, 0.0, pltpu.roll(value, cz - step, 1))
        return low + high

    def stencil(field, i, count, row, rows, step):
        planes = [field[i + k, pl.ds(row, rows), :] for k in range(-1, count + 1)]
        sums = []
        for k in range(count):
            total = planes[k] + planes[k + 2] + lanes(planes[k + 1], step)
            total = total + (field[i + k, pl.ds(row - 1, rows), :] + field[i + k, pl.ds(row + 1, rows), :])
            sums.append(total)
        return planes[1:-1], sums

    def in_groups(low, high, size, one):
        whole = (high - low) // size

        def body(g, carry):
            one(low + g * size, size, low)
            return carry

        lax.fori_loop(0, whole, body, 0)
        if (high - low) % size:
            one(low + whole * size, (high - low) % size, low)

    def smooth(field, count, bands):
        for t in range(2 * count):
            reach = 2 * count - t

            def one(i, size, low):
                stores = []
                for row, rows, limit in bands:
                    centres, sums = stencil(field, i, size, row, rows, 1)
                    allowed = limit(t)
                    for k in range(size):
                        at = i + k
                        region = region_of(at, DEPTH, cx)
                        parity = (low + k + DEPTH + t) % 2
                        mask = weights[region, parity, pl.ds(row - 8, rows), :] > 0.5
                        if allowed is not None:
                            mask = mask & allowed
                        update = (rhs[at, pl.ds(row, rows), :] - mean + sums[k]) * (1.0 / 6.0)
                        stores.append((at, row, rows, jnp.where(mask, update, centres[k])))
                for at, row, rows, value in stores:
                    field[at, pl.ds(row, rows), :] = value

            in_groups(DEPTH - reach, DEPTH + cx + reach, GROUP, one)

    edge = 2 * SWEEP_DEPTH
    inner_row = lax.broadcasted_iota(jnp.int32, (cy - 2, cz), 0) + 1
    edge_row = lax.broadcasted_iota(jnp.int32, (edge, cz), 0) - SWEEP_DEPTH
    smooth(fine, PRE, [(ROW0 + 1, cy - 2, lambda t: (inner_row > t) & (inner_row < cy - 1 - t))])
    arrive(first_round, [side for side in SIDES if side not in along])
    fine_masks(-SWEEP_DEPTH, SWEEP_DEPTH, 0)
    fine_masks(cy, SWEEP_DEPTH, 2)
    smooth(fine, PRE, [
        (ROW0 - SWEEP_DEPTH, edge, lambda t: edge_row <= t),
        (ROW0 + cy - SWEEP_DEPTH, edge, lambda t: edge_row >= -1 - t),
    ])

    lane = lax.broadcasted_iota(jnp.int32, (cy, cz), 1)
    even = lane % 2 == 0

    def defects(field, i, count):
        centres, sums = stencil(field, i, count, ROW0, cy, 1)
        return centres, [rhs[i + k, own_rows, :] - mean - (6.0 * centres[k] - sums[k]) for k in range(count)]

    def restrict(a, size, low):
        i = DEPTH + 2 * a
        centres, res = defects(fine, i, 2 * size)
        for k in range(size):
            both = res[2 * k] + res[2 * k + 1]
            both = both + jnp.where(even, pltpu.roll(both, cz - 1, 1), pltpu.roll(both, 1, 1))
            pair_rows[a + k] = both
        for k in range(2 * size):
            post[i + k, own_rows, :] = centres[k]
            post[i + k, pl.ds(ROW0 - 1, 1), :] = fine[i + k, pl.ds(ROW0 - 1, 1), :]
            post[i + k, pl.ds(ROW0 + cy, 1), :] = fine[i + k, pl.ds(ROW0 + cy, 1), :]
        for k in range(size):
            coarse[COARSE_DEPTH + a + k, pl.ds(COARSE_ROW0, hy), :] = 0.5 * (
                pair_rows[a + k, pl.ds(0, hy, stride=2), :] + pair_rows[a + k, pl.ds(1, hy, stride=2), :]
            )

    in_groups(0, hx, 2, restrict)

    leven = lax.broadcasted_iota(jnp.int32, (COARSE_DEPTH, cz), 1) % 2 == 0
    for dy in (-1, 1):
        sy = slabs(dy, hy, COARSE_ROW0, 0, COARSE_DEPTH)[0]
        for k in range(half_planes):
            packed[1 + dy, k] = jnp.where(
                leven, coarse[COARSE_DEPTH + k, sy, :], coarse[COARSE_DEPTH + half_planes + k, sy, :]
            )

    start(second_coarse)
    for i in (DEPTH - 1, DEPTH + cx):
        post[i, own_rows, :] = fine[i, own_rows, :]
    start(second_fine)
    arrive(second_coarse)
    sent(second_coarse)
    for dy in (-1, 1):
        ty = slabs(dy, hy, COARSE_ROW0, 0, COARSE_DEPTH)[1]

        @pl.when(there(0, -dy))
        def _():
            for k in range(half_planes):
                both = packed[1 + dy, half_planes + k]
                coarse[COARSE_DEPTH + k, ty, :] = jnp.where(leven, both, pltpu.roll(both, 1, 1))
                coarse[COARSE_DEPTH + half_planes + k, ty, :] = jnp.where(leven, pltpu.roll(both, cz - 1, 1), both)

    planes = hx + 2 * COARSE_DEPTH

    def coarse_mask(at, parity):
        return coarse_weights[region_of(at, COARSE_DEPTH, hx), parity % 2] > 0.5

    def coarse_first(i, size, low):
        for k in range(size):
            start_value = coarse[i + k, pl.ds(8, coarse_work), :] * (1.0 / 6.0)
            mask = coarse_mask(i + k, low + k + COARSE_DEPTH)
            corr[i + k, pl.ds(8, coarse_work), :] = jnp.where(mask, start_value, 0.0)

    in_groups(0, planes, GROUP, coarse_first)
    for t in range(1, 2 * COARSE):
        def coarse_one(i, size, low):
            centres, sums = stencil(corr, i, size, 8, coarse_work, 2)
            fresh = []
            for k in range(size):
                update = (coarse[i + k, pl.ds(8, coarse_work), :] + sums[k]) * (1.0 / 6.0)
                fresh.append(jnp.where(coarse_mask(i + k, low + k + COARSE_DEPTH + t), update, centres[k]))
            for k in range(size):
                corr[i + k, pl.ds(8, coarse_work), :] = fresh[k]

        in_groups(t, planes - t, GROUP, coarse_one)

    arrive(second_fine)
    sent(second_fine)

    half_rows = hy + 8
    first_plane = 2 * COARSE - 1

    def add_correction(c, size, low, sides=(0, 1)):
        for k in range(size):
            plane = corr[c + k, pl.ds(COARSE_ROW0 - 4, half_rows), :]
            wide_rows[c + k, pl.ds(0, half_rows, stride=2), :] = plane
            wide_rows[c + k, pl.ds(1, half_rows, stride=2), :] = plane
        rows = pl.ds(ROW0 - 8, cy + 16)
        fresh = []
        for k in range(size):
            wide = wide_rows[c + k]
            for b in sides:
                i = 2 * (c + k - COARSE_DEPTH) + DEPTH + b
                fresh.append((i, post[i, rows, :] + wide))
        for i, value in fresh:
            post[i, rows, :] = value

    add_correction(first_plane, 1, 0, (1,))
    in_groups(first_plane + 1, planes - first_plane - 1, 2, add_correction)
    add_correction(planes - first_plane - 1, 1, 0, (0,))

    smooth(post, POST, [(8, work, lambda t: None)])
    store_smoothed = pltpu.make_async_copy(post.at[own_planes, own_rows], smoothed_ref, local_sem.at[0])
    store_smoothed.start()
    sent(first_round)

    def last(i, size, low):
        for k, value in enumerate(defects(post, DEPTH + i, size)[1]):
            res_rows[i + k] = value

    in_groups(0, cx, GROUP, last)
    store_residual = pltpu.make_async_copy(res_rows, residual_ref, local_sem.at[1])
    store_residual.start()
    for c in msum + gsum:
        c.wait_send()
    store_smoothed.wait()
    store_residual.wait()


def per_device(dims, source, potential, refined):
    cx, cy, cz = source.shape
    groups, members = dims
    hx, hy = cx // 2, cy // 2
    wide = (cx + 2 * DEPTH, ROW0 + cy + ROW0, cz)
    narrow = (hx + 2 * COARSE_DEPTH, hy + 2 * COARSE_ROW0, cz)
    f32 = jnp.float32
    dma = pltpu.SemaphoreType.DMA
    any_spec = pl.BlockSpec(memory_space=pl.ANY)
    return tuple(pl.pallas_call(
        functools.partial(kernel, dims, (cx, cy, cz)),
        out_shape=[jax.ShapeDtypeStruct(source.shape, f32)] * 2,
        in_specs=[pl.BlockSpec(memory_space=pltpu.SMEM), any_spec, any_spec],
        out_specs=[any_spec, any_spec],
        scratch_shapes=[
            pltpu.VMEM(wide, f32),
            pltpu.VMEM(wide, f32),
            pltpu.VMEM(wide, f32),
            pltpu.VMEM(narrow, f32),
            pltpu.VMEM(narrow, f32),
            pltpu.VMEM((3, 2 * (hx // 2), COARSE_DEPTH, cz), f32),
            pltpu.VMEM((3, 3, 8, cz), f32),
            pltpu.VMEM((3, 2, cy + 2 * SWEEP_DEPTH, cz), f32),
            pltpu.VMEM((3, 2, hy + 16, cz), f32),
            pltpu.VMEM((hx, cy, cz), f32),
            pltpu.VMEM((narrow[0], cy + 16, cz), f32),
            pltpu.VMEM((cx, cy, cz), f32),
            pltpu.VMEM((members, 8, cz), f32),
            pltpu.VMEM((groups, 8, cz), f32),
            dma((3,)),
            dma((1 + 4 * STEPS, len(SIDES))),
            dma((1 + 4 * STEPS, len(SIDES))),
            dma((members,)),
            dma((members,)),
            dma((groups,)),
            dma((groups,)),
        ],
        compiler_params=pltpu.CompilerParams(collective_id=0, has_side_effects=True),
    )(refined, source, potential))


def solution(mesh):
    spec = P("group", "member", None)
    return jax.shard_map(
        functools.partial(per_device, (mesh.shape["group"], mesh.shape["member"])),
        mesh=mesh,
        in_specs=(spec, spec, spec),
        out_specs=(spec, spec),
        check_vma=False,
    )
```
